32 devices in a mesh: sub: 8 (over z, core), sta: 4 (over y, x).
Axes of the slice: x: 2, y: 2, z: 4, core: 2. Of those that a mesh axis runs over, the one named last changes fastest.
Arguments:
- voltages: bfloat16 [8, 2, 64, 65536], P('sub', None, 'sta'), may hold values from -6 to 6
- beam_weights: bfloat16 [8, 2, 32, 64], P('sub'), may hold values from -0.5 to 0.5
- station_delays: int32 [64], P('sta'), may hold values from 0 to 16383
- dm_index: int32 [32, 1], P('sta'), may hold values from 1 to 8
Outputs:
- dedispersed: float32 [8, 2, 32, 1, 65536], P(None, None, None, None, ('sub', 'sta'))
- intensity: float32 [32, 1, 65536], P(None, None, ('sub', 'sta'))
The draws below stay inside these ranges and needn't reach their ends.
Inputs may be any that keep to these rules, and one draw needn't show every extreme that they name: `station_delays`: delays in whole samples. `dm_index`: dispersion measure in steps of 10.
All inputs are finite; a program needn't handle non-finite values.
Results may differ from the reference program's by a relative error of at most 0.0006.
Values may be sent and summed in bfloat16 or wider, within the bound.
A program may use at most 320 MiB of HBM per device.

```python
import jax
import jax.numpy as jnp
from jax import lax

STATIONS = 64
BEAMS = 32
DMS = 1
SAMPLES = 65536
SUBBANDS = 8


def set_ends(values, key, low, largest):
    extent = values.shape
    spot = [jax.random.randint(jax.random.fold_in(key, axis), (), 0, extent[axis]) for axis in range(len(extent))]
    values = values.at[tuple(spot)].set(low)
    longest = extent.index(max(extent))
    spot[longest] = (spot[longest] + 1) % extent[longest]
    return values.at[tuple(spot)].set(largest)


def block_scale(rng, shape, split, low, top_value):
    def one(axis_at, shards_of):
        heights = jax.random.uniform(jax.random.fold_in(jax.random.fold_in(rng, 6), axis_at), (shards_of,), jnp.float32, low / len(split), top_value / len(split))
        return jnp.repeat(jnp.exp(heights), shape[axis_at] // shards_of).reshape((-1,) + (1,) * (len(shape) - axis_at - 1))

    gain = one(*split[0])
    for cut in split[1:]:
        gain = gain * one(*cut)
    return gain


def bell_draw(own_key, dims, scale, limit, pieces=(), kind=jnp.bfloat16):
    drawn = jax.random.normal(own_key, dims, jnp.float32) * scale
    if len(pieces) > 0:
        drawn = block_scale(own_key, dims, pieces, -0.22, 0.18) * drawn
    return jnp.clip(drawn, min=-limit, max=limit).astype(kind)


def setup_inputs(seed: int = 0) -> dict:
    streams_of = jax.random.split(jax.random.key(seed), 5)
    voltages = bell_draw(streams_of[0], (SUBBANDS, 2, STATIONS, SAMPLES), 1.0, 6.0, ((0, 8), (2, 4)))
    beam_weights = bell_draw(streams_of[1], (SUBBANDS, 2, BEAMS, STATIONS), (2 * STATIONS) ** -0.5, 0.5, ((0, 8),))
    station_delays = set_ends(jax.random.randint(streams_of[2], (STATIONS,), 0, SAMPLES // 4), jax.random.fold_in(streams_of[2], 1), 0, (SAMPLES // 4) - 1).astype(jnp.int32)
    dm_index = set_ends(jax.random.randint(streams_of[3], (BEAMS, DMS), 1, 9), jax.random.fold_in(streams_of[3], 1), 1, 8).astype(jnp.int32)
    return dict(voltages=voltages, beam_weights=beam_weights, station_delays=station_delays, dm_index=dm_index)


TWO_PI = 6.283185307179586
DISPERSION = 4148808000.0
DM_STEP = 10.0
BASE_FREQ = 120.0
CHANNEL_WIDTH = 0.1953125


def chirp_base(subband, total_len):
    positions = jnp.arange(total_len, dtype=jnp.int32)
    signed_bin = jnp.where(positions < total_len // 2, positions, positions - total_len)
    offset = CHANNEL_WIDTH * signed_bin.astype(jnp.float32) / total_len
    centre = BASE_FREQ + CHANNEL_WIDTH * (subband.astype(jnp.float32) + 0.5)
    return TWO_PI * DISPERSION * offset * offset / (centre * centre * (centre + offset))


def reference(voltages, beam_weights, station_delays, dm_index):
    dm_value = DM_STEP * dm_index.astype(jnp.float32)

    def one_subband(inputs):
        subband, volts, weights = inputs
        shifted = jax.vmap(lambda rows, shift_by: jnp.roll(rows, shift_by, axis=-1), in_axes=(1, 0), out_axes=1)(volts, station_delays)
        real_part = jnp.dot(weights[0], shifted[0], preferred_element_type=jnp.float32) - jnp.dot(weights[1], shifted[1], preferred_element_type=jnp.float32)
        imag_part = jnp.dot(weights[0], shifted[1], preferred_element_type=jnp.float32) + jnp.dot(weights[1], shifted[0], preferred_element_type=jnp.float32)
        spectrum = jnp.fft.fft(lax.complex(real_part, imag_part), axis=-1)
        phase_table = dm_value[:, :, None] * chirp_base(subband, SAMPLES)[None, None, :]
        chirped = spectrum[:, None, :] * lax.complex(jnp.cos(phase_table), jnp.sin(phase_table))
        series = jnp.fft.ifft(chirped, axis=-1)
        return jnp.stack([jnp.real(series), jnp.imag(series)], axis=0)

    dedispersed = lax.map(one_subband, (jnp.arange(SUBBANDS, dtype=jnp.int32), voltages, beam_weights))
    intensity = jnp.mean(dedispersed[:, 0] * dedispersed[:, 0] + dedispersed[:, 1] * dedispersed[:, 1], axis=0)
    return dedispersed, intensity
```

```python
import functools

import jax
import jax.numpy as jnp
import numpy as np
from jax import lax
from jax.experimental import pallas as pl
from jax.experimental.pallas import tpu as pltpu
from jax.sharding import PartitionSpec as P


TWO_PI = 6.283185307179586
DISPERSION = 4148808000.0
DM_STEP = 10.0
BASE_FREQ = 120.0
CHANNEL_WIDTH = 0.1953125


def dft_tables(root_len):
    total_len = root_len * root_len
    product = np.outer(np.arange(root_len), np.arange(root_len))
    root_angle = 2 * np.pi * (product % root_len) / root_len
    cos_root, sin_root = np.cos(root_angle), np.sin(root_angle)
    left = np.block([[cos_root, sin_root], [-sin_root, cos_root]]).astype(np.float32)
    high = left.astype(jnp.bfloat16)
    low = (left - high.astype(np.float32)).astype(jnp.bfloat16)
    twist_angle = 2 * np.pi * product / total_len
    twist = np.stack([np.cos(twist_angle), np.sin(twist_angle)]).astype(np.float32)
    return np.stack([high, low]), np.stack([high.T, low.T]), twist


def chirp_base(subband, root_len, total_len):
    first = jnp.arange(root_len, dtype=jnp.int32)[:, None]
    second = jnp.arange(root_len, dtype=jnp.int32)[None, :]
    positions = first + root_len * second
    signed_bin = jnp.where(positions < total_len // 2, positions, positions - total_len)
    offset = (CHANNEL_WIDTH * signed_bin.astype(jnp.float32) / total_len)[None]
    centre = (BASE_FREQ + CHANNEL_WIDTH * (subband.astype(jnp.float32) + 0.5))[:, None, None]
    return TWO_PI * DISPERSION * offset * offset / (centre * centre * (centre + offset))


def beam_kernel(w_ref, v_ref, out_ref):
    sums = jnp.dot(w_ref[...], v_ref[...], preferred_element_type=jnp.float32)
    lanes = out_ref.shape[2]
    for row in range(out_ref.shape[1]):
        out_ref[:, row, :] = sums[:, row * lanes : (row + 1) * lanes]


def form_beams(weights, volts, root_len):
    rows, depth = weights.shape
    total_len = volts.shape[1]
    step = 32
    return pl.pallas_call(
        beam_kernel,
        grid=(root_len // step,),
        in_specs=[
            pl.BlockSpec((rows, depth), lambda i: (0, 0)),
            pl.BlockSpec((depth, step * root_len), lambda i: (0, i)),
        ],
        out_specs=pl.BlockSpec((rows, step, root_len), lambda i: (0, i, 0)),
        out_shape=jax.ShapeDtypeStruct((rows, root_len, root_len), jnp.float32),
        cost_estimate=pl.CostEstimate(
            flops=2 * rows * depth * total_len, bytes_accessed=2 * depth * total_len, transcendentals=0
        ),
    )(weights, volts)


def split(values):
    high = values.astype(jnp.bfloat16)
    return high, (values - high.astype(jnp.float32)).astype(jnp.bfloat16)


def dot3(a_high, a_low, b_high, b_low):
    dot = functools.partial(jnp.dot, preferred_element_type=jnp.float32)
    return dot(a_high, b_high) + (dot(a_high, b_low) + dot(a_low, b_high))


def dedisperse_kernel(x_ref, h_real_ref, h_imag_ref, left_ref, right_ref, twist_ref, out_ref, flat):
    root = twist_ref.shape[1]
    half = root // 2
    cos_twist, sin_twist = twist_ref[0], twist_ref[1]
    x = x_ref[...].reshape(2 * root, root)
    a = dot3(left_ref[0], left_ref[1], *split(x))
    a_real, a_imag = a[:root], a[root:]
    b = jnp.concatenate(
        [a_real * cos_twist + a_imag * sin_twist, a_imag * cos_twist - a_real * sin_twist], axis=1
    )
    s = dot3(*split(b), right_ref[0], right_ref[1])
    s_real, s_imag = s[:, :root], s[:, root:]
    h_real, h_imag = h_real_ref[0], h_imag_ref[0]
    c = jnp.concatenate([s_real * h_real - s_imag * h_imag, s_real * h_imag + s_imag * h_real], axis=1)
    d = dot3(*split(c), left_ref[0], left_ref[1])
    d_real, d_imag = d[:, :root], d[:, root:]
    e = jnp.concatenate(
        [d_real * cos_twist - d_imag * sin_twist, d_imag * cos_twist + d_real * sin_twist], axis=0
    )
    out = dot3(right_ref[0], right_ref[1], *split(e)) * (1.0 / (root * root))
    for part in range(2):
        for side in range(2):
            flat[pl.ds(side, root, 2), :] = out[part * root : (part + 1) * root, side * half : (side + 1) * half]
        out_ref[:, part, 0] = flat[...].reshape(out_ref.shape[0], out_ref.shape[3], half)


def dedisperse(beams, h_real, h_imag, n_dev):
    _, n_beams, root, _ = beams.shape
    left, right, twist = dft_tables(root)
    rows = 2 * root // n_dev
    whole = lambda shape: pl.BlockSpec(shape, lambda b: (0,) * len(shape))
    own = pl.BlockSpec((1, root, root), lambda b: (b, 0, 0))
    return pl.pallas_call(
        dedisperse_kernel,
        grid=(n_beams,),
        in_specs=[
            pl.BlockSpec((2, 1, root, root), lambda b: (0, b, 0, 0)),
            own,
            own,
            whole(left.shape),
            whole(right.shape),
            whole(twist.shape),
        ],
        out_specs=pl.BlockSpec((n_dev, 2, 1, rows, root // 2), lambda b: (0, 0, b, 0, 0)),
        out_shape=jax.ShapeDtypeStruct((n_dev, 2, n_beams, rows, root // 2), jnp.float32),
        scratch_shapes=[pltpu.VMEM((2 * root, root // 2), jnp.float32)],
        cost_estimate=pl.CostEstimate(
            flops=96 * n_beams * root**3, bytes_accessed=24 * n_beams * root**2, transcendentals=0
        ),
    )(beams, h_real, h_imag, left, right, twist)


def shards(voltages, beam_weights, station_delays, dm_index):
    sub_dev = voltages.shape[0]
    total_len = voltages.shape[3]
    local_beams = dm_index.shape[0]
    trials = dm_index.shape[1]
    root_len = int(round(total_len**0.5))
    n_sub = lax.axis_size("sub")
    n_sta = lax.axis_size("sta")
    n_dev = n_sub * n_sta
    assert sub_dev == 1 and trials == 1 and root_len * root_len == total_len
    doubled = jnp.concatenate([voltages, voltages], axis=3)
    shifted = jax.vmap(
        lambda rows, shift_by: lax.dynamic_slice_in_dim(rows, total_len - shift_by, total_len, 2),
        in_axes=(2, 0),
        out_axes=2,
    )(doubled, station_delays)
    own_weights = lax.dynamic_slice_in_dim(
        beam_weights, lax.axis_index("sta") * local_beams, local_beams, 2
    )[0]
    w_real, w_imag = own_weights[0], own_weights[1]
    volts = lax.all_gather(shifted[0], "sta", axis=1, tiled=True)
    volts = volts.reshape(-1, total_len)
    weights = jnp.concatenate(
        [jnp.concatenate([w_real, -w_imag], axis=1), jnp.concatenate([w_imag, w_real], axis=1)], axis=0
    )
    beams = form_beams(weights, volts, root_len).reshape(2, local_beams, root_len, root_len)
    subband = lax.axis_index("sub") + jnp.arange(1, dtype=jnp.int32)
    base_phase = chirp_base(subband, root_len, total_len)
    dm_value = DM_STEP * dm_index.astype(jnp.float32)
    phase_table = dm_value[:, :, None] * base_phase
    sent = dedisperse(beams, jnp.cos(phase_table), jnp.sin(phase_table), n_dev)
    moved = lax.all_to_all(sent, ("sub", "sta"), split_axis=0, concat_axis=0, tiled=True)
    moved = moved.reshape(n_sub, n_sta, *moved.shape[1:]).transpose(0, 2, 1, 3, 4, 5)
    moved = moved.reshape(n_sub, 2, n_sta * local_beams, *moved.shape[4:])
    intensity = jnp.mean(moved[:, 0] * moved[:, 0] + moved[:, 1] * moved[:, 1], axis=0)
    return (moved.reshape(*moved.shape[:3], 1, -1), intensity.reshape(intensity.shape[0], 1, -1))


def solution(mesh):
    return jax.shard_map(
        shards,
        mesh=mesh,
        in_specs=(
            P("sub", None, "sta", None),
            P("sub", None, None, None),
            P("sta"),
            P("sta", None),
        ),
        out_specs=(P(None, None, None, None, ("sub", "sta")), P(None, None, ("sub", "sta"))),
        check_vma=False,
    )
```

```python
import functools

import jax
import jax.numpy as jnp
import numpy as np
from jax import lax
from jax.experimental import pallas as pl
from jax.experimental.pallas import tpu as pltpu
from jax.sharding import PartitionSpec as P


TWO_PI = 6.283185307179586
DISPERSION = 4148808000.0
DM_STEP = 10.0
BASE_FREQ = 120.0
CHANNEL_WIDTH = 0.1953125


def dft_tables(root_len):
    total_len = root_len * root_len
    product = np.outer(np.arange(root_len), np.arange(root_len))
    root_angle = 2 * np.pi * (product % root_len) / root_len
    cos_root, sin_root = np.cos(root_angle), np.sin(root_angle)
    left = np.block([[cos_root, sin_root], [-sin_root, cos_root]]).astype(np.float32)
    high = left.astype(jnp.bfloat16)
    low = (left - high.astype(np.float32)).astype(jnp.bfloat16)
    twist_angle = 2 * np.pi * product / total_len
    twist = np.stack([np.cos(twist_angle), np.sin(twist_angle)]).astype(np.float32)
    return np.stack([high, low]), np.stack([high.T, low.T]), twist


def chirp_base(subband, root_len, total_len):
    first = jnp.arange(root_len, dtype=jnp.int32)[:, None]
    second = jnp.arange(root_len, dtype=jnp.int32)[None, :]
    positions = first + root_len * second
    signed_bin = jnp.where(positions < total_len // 2, positions, positions - total_len)
    offset = (CHANNEL_WIDTH * signed_bin.astype(jnp.float32) / total_len)[None]
    centre = (BASE_FREQ + CHANNEL_WIDTH * (subband.astype(jnp.float32) + 0.5))[:, None, None]
    return TWO_PI * DISPERSION * offset * offset / (centre * centre * (centre + offset))


def beam_kernel(w_ref, v_ref, out_ref):
    sums = jnp.dot(w_ref[...], v_ref[...], preferred_element_type=jnp.float32)
    lanes = out_ref.shape[2]
    for row in range(out_ref.shape[1]):
        out_ref[:, row, :] = sums[:, row * lanes : (row + 1) * lanes]


def form_beams(weights, volts, root_len):
    rows, depth = weights.shape
    total_len = volts.shape[1]
    step = 32
    return pl.pallas_call(
        beam_kernel,
        grid=(root_len // step,),
        in_specs=[
            pl.BlockSpec((rows, depth), lambda i: (0, 0)),
            pl.BlockSpec((depth, step * root_len), lambda i: (0, i)),
        ],
        out_specs=pl.BlockSpec((rows, step, root_len), lambda i: (0, i, 0)),
        out_shape=jax.ShapeDtypeStruct((rows, root_len, root_len), jnp.float32),
        cost_estimate=pl.CostEstimate(
            flops=2 * rows * depth * total_len, bytes_accessed=2 * depth * total_len, transcendentals=0
        ),
    )(weights, volts)


def shift_kernel(delay_ref, x_ref, out_ref, doubled, window):
    rows, total_len = x_ref.shape[1:]
    width = window.shape[1]
    step = width - 128
    doubled[:, :total_len] = x_ref[0].astype(jnp.float32)
    doubled[:, total_len:] = doubled[:, :total_len]
    row_id = lax.broadcasted_iota(jnp.int32, (rows, width), 0)
    fine = jnp.zeros((rows, width), jnp.int32)
    for row in range(rows):
        fine = jnp.where(row_id == row, delay_ref[row] % 128, fine)

    def chunk(i, carry):
        for row in range(rows):
            start = total_len + i * step - (delay_ref[row] // 128) * 128 - 128
            window[row : row + 1, :] = doubled[row : row + 1, pl.ds(pl.multiple_of(start, 128), width)]
        values = window[...]
        for bit in range(7):
            values = jnp.where((fine >> bit) & 1 == 1, pltpu.roll(values, 1 << bit, 1), values)
        out_ref[0, :, pl.ds(pl.multiple_of(i * step, 128), step)] = values[:, 128:].astype(out_ref.dtype)
        return carry

    lax.fori_loop(0, total_len // step, chunk, 0)


def shift(volts, delays):
    parts, rows, total_len = volts.shape
    block = pl.BlockSpec((1, rows, total_len), lambda i: (i, 0, 0))
    return pl.pallas_call(
        shift_kernel,
        grid=(parts,),
        in_specs=[pl.BlockSpec(memory_space=pltpu.SMEM), block],
        out_specs=block,
        out_shape=jax.ShapeDtypeStruct(volts.shape, volts.dtype),
        scratch_shapes=[
            pltpu.VMEM((rows, 2 * total_len), jnp.float32),
            pltpu.VMEM((rows, 2048 + 128), jnp.float32),
        ],
    )(delays, volts)


def split(values):
    high = values.astype(jnp.bfloat16)
    return high, (values - high.astype(jnp.float32)).astype(jnp.bfloat16)


def dot3(a_high, a_low, b_high, b_low):
    dot = functools.partial(jnp.dot, preferred_element_type=jnp.float32)
    return dot(a_high, b_high) + (dot(a_high, b_low) + dot(a_low, b_high))


def dedisperse_kernel(x_ref, h_real_ref, h_imag_ref, left_ref, right_ref, twist_ref, out_ref, flat):
    root = twist_ref.shape[1]
    half = root // 2
    cos_twist, sin_twist = twist_ref[0], twist_ref[1]
    x = x_ref[...].reshape(2 * root, root)
    a = dot3(left_ref[0], left_ref[1], *split(x))
    a_real, a_imag = a[:root], a[root:]
    b = jnp.concatenate(
        [a_real * cos_twist + a_imag * sin_twist, a_imag * cos_twist - a_real * sin_twist], axis=1
    )
    s = dot3(*split(b), right_ref[0], right_ref[1])
    s_real, s_imag = s[:, :root], s[:, root:]
    h_real, h_imag = h_real_ref[0], h_imag_ref[0]
    c = jnp.concatenate([s_real * h_real - s_imag * h_imag, s_real * h_imag + s_imag * h_real], axis=1)
    d = dot3(*split(c), left_ref[0], left_ref[1])
    d_real, d_imag = d[:, :root], d[:, root:]
    e = jnp.concatenate(
        [d_real * cos_twist - d_imag * sin_twist, d_imag * cos_twist + d_real * sin_twist], axis=0
    )
    out = dot3(right_ref[0], right_ref[1], *split(e)) * (1.0 / (root * root))
    for part in range(2):
        for side in range(2):
            flat[pl.ds(side, root, 2), :] = out[part * root : (part + 1) * root, side * half : (side + 1) * half]
        out_ref[:, part, 0] = flat[...].reshape(out_ref.shape[0], out_ref.shape[3], half)


def dedisperse(beams, h_real, h_imag, n_dev):
    _, n_beams, root, _ = beams.shape
    left, right, twist = dft_tables(root)
    rows = 2 * root // n_dev
    whole = lambda shape: pl.BlockSpec(shape, lambda b: (0,) * len(shape))
    own = pl.BlockSpec((1, root, root), lambda b: (b, 0, 0))
    return pl.pallas_call(
        dedisperse_kernel,
        grid=(n_beams,),
        in_specs=[
            pl.BlockSpec((2, 1, root, root), lambda b: (0, b, 0, 0)),
            own,
            own,
            whole(left.shape),
            whole(right.shape),
            whole(twist.shape),
        ],
        out_specs=pl.BlockSpec((n_dev, 2, 1, rows, root // 2), lambda b: (0, 0, b, 0, 0)),
        out_shape=jax.ShapeDtypeStruct((n_dev, 2, n_beams, rows, root // 2), jnp.float32),
        scratch_shapes=[pltpu.VMEM((2 * root, root // 2), jnp.float32)],
        cost_estimate=pl.CostEstimate(
            flops=96 * n_beams * root**3, bytes_accessed=24 * n_beams * root**2, transcendentals=0
        ),
    )(beams, h_real, h_imag, left, right, twist)


def shards(voltages, beam_weights, station_delays, dm_index):
    sub_dev = voltages.shape[0]
    total_len = voltages.shape[3]
    local_beams = dm_index.shape[0]
    trials = dm_index.shape[1]
    root_len = int(round(total_len**0.5))
    n_sub = lax.axis_size("sub")
    n_sta = lax.axis_size("sta")
    n_dev = n_sub * n_sta
    assert sub_dev == 1 and trials == 1 and root_len * root_len == total_len
    shifted = shift(voltages[0], station_delays)
    own_weights = lax.dynamic_slice_in_dim(
        beam_weights, lax.axis_index("sta") * local_beams, local_beams, 2
    )[0]
    w_real, w_imag = own_weights[0], own_weights[1]
    volts = lax.all_gather(shifted, "sta", axis=1, tiled=True)
    volts = volts.reshape(-1, total_len)
    weights = jnp.concatenate(
        [jnp.concatenate([w_real, -w_imag], axis=1), jnp.concatenate([w_imag, w_real], axis=1)], axis=0
    )
    beams = form_beams(weights, volts, root_len).reshape(2, local_beams, root_len, root_len)
    subband = lax.axis_index("sub") + jnp.arange(1, dtype=jnp.int32)
    base_phase = chirp_base(subband, root_len, total_len)
    dm_value = DM_STEP * dm_index.astype(jnp.float32)
    phase_table = dm_value[:, :, None] * base_phase
    sent = dedisperse(beams, jnp.cos(phase_table), jnp.sin(phase_table), n_dev)
    power = jnp.mean(beams[0] * beams[0] + beams[1] * beams[1], axis=(1, 2))
    rms = jnp.where(power > 0, jnp.sqrt(power), 1.0)
    gain = 32768.0 / root_len / rms
    undo = lax.all_gather(rms * (root_len / 32768.0), ("sub", "sta"), axis=0)
    sent = (sent * gain[None, None, :, None, None]).astype(jnp.float16)
    moved = lax.all_to_all(sent, ("sub", "sta"), split_axis=0, concat_axis=0, tiled=True)
    moved = moved.astype(jnp.float32) * undo[:, None, :, None, None]
    moved = moved.reshape(n_sub, n_sta, *moved.shape[1:]).transpose(0, 2, 1, 3, 4, 5)
    moved = moved.reshape(n_sub, 2, n_sta * local_beams, *moved.shape[4:])
    intensity = jnp.mean(moved[:, 0] * moved[:, 0] + moved[:, 1] * moved[:, 1], axis=0)
    return (moved.reshape(*moved.shape[:3], 1, -1), intensity.reshape(intensity.shape[0], 1, -1))


def solution(mesh):
    return jax.shard_map(
        shards,
        mesh=mesh,
        in_specs=(
            P("sub", None, "sta", None),
            P("sub", None, None, None),
            P("sta"),
            P("sta", None),
        ),
        out_specs=(P(None, None, None, None, ("sub", "sta")), P(None, None, ("sub", "sta"))),
        check_vma=False,
    )
```

```python
import functools

import jax
import jax.numpy as jnp
import numpy as np
from jax import lax
from jax.experimental import pallas as pl
from jax.experimental.pallas import tpu as pltpu
from jax.sharding import PartitionSpec as P


TWO_PI = 6.283185307179586
DISPERSION = 4148808000.0
DM_STEP = 10.0
BASE_FREQ = 120.0
CHANNEL_WIDTH = 0.1953125


def dft_tables(root_len):
    total_len = root_len * root_len
    product = np.outer(np.arange(root_len), np.arange(root_len))
    root_angle = 2 * np.pi * (product % root_len) / root_len
    cos_root, sin_root = np.cos(root_angle), np.sin(root_angle)
    left = np.block([[cos_root, sin_root], [-sin_root, cos_root]]).astype(np.float32)
    high = left.astype(jnp.bfloat16)
    low = (left - high.astype(np.float32)).astype(jnp.bfloat16)
    twist_angle = 2 * np.pi * product / total_len
    twist = np.stack([np.cos(twist_angle), np.sin(twist_angle)]).astype(np.float32)
    return np.stack([high, low]), np.stack([high.T, low.T]), twist


def chirp_base(subband, root_len, total_len):
    first = jnp.arange(root_len, dtype=jnp.int32)[:, None]
    second = jnp.arange(root_len, dtype=jnp.int32)[None, :]
    positions = first + root_len * second
    signed_bin = jnp.where(positions < total_len // 2, positions, positions - total_len)
    offset = (CHANNEL_WIDTH * signed_bin.astype(jnp.float32) / total_len)[None]
    centre = (BASE_FREQ + CHANNEL_WIDTH * (subband.astype(jnp.float32) + 0.5))[:, None, None]
    return TWO_PI * DISPERSION * offset * offset / (centre * centre * (centre + offset))


def beam_kernel(w_ref, v_real_ref, v_imag_ref, out_ref):
    sums = jnp.dot(w_ref[0], v_real_ref[...], preferred_element_type=jnp.float32)
    sums += jnp.dot(w_ref[1], v_imag_ref[...], preferred_element_type=jnp.float32)
    lanes = out_ref.shape[2]
    for row in range(out_ref.shape[1]):
        out_ref[:, row, :] = sums[:, row * lanes : (row + 1) * lanes]


def form_beams(weights, v_real, v_imag, root_len):
    _, rows, depth = weights.shape
    total_len = v_real.shape[1]
    step = 32
    return pl.pallas_call(
        beam_kernel,
        grid=(root_len // step,),
        in_specs=[
            pl.BlockSpec((2, rows, depth), lambda i: (0, 0, 0)),
            pl.BlockSpec((depth, step * root_len), lambda i: (0, i)),
            pl.BlockSpec((depth, step * root_len), lambda i: (0, i)),
        ],
        out_specs=pl.BlockSpec((rows, step, root_len), lambda i: (0, i, 0)),
        out_shape=jax.ShapeDtypeStruct((rows, root_len, root_len), jnp.float32),
        cost_estimate=pl.CostEstimate(
            flops=2 * rows * depth * total_len, bytes_accessed=2 * depth * total_len, transcendentals=0
        ),
    )(weights, v_real, v_imag)


def shift_kernel(delay_ref, x_ref, out_ref, doubled, window):
    rows, total_len = x_ref.shape[1:]
    width = window.shape[1]
    step = width - 128
    doubled[:, :total_len] = x_ref[0].astype(jnp.float32)
    doubled[:, total_len:] = doubled[:, :total_len]
    row_id = lax.broadcasted_iota(jnp.int32, (rows, width), 0)
    fine = jnp.zeros((rows, width), jnp.int32)
    for row in range(rows):
        fine = jnp.where(row_id == row, delay_ref[row] % 128, fine)

    def chunk(i, carry):
        for row in range(rows):
            start = total_len + i * step - (delay_ref[row] // 128) * 128 - 128
            window[row : row + 1, :] = doubled[row : row + 1, pl.ds(pl.multiple_of(start, 128), width)]
        values = window[...]
        for bit in range(7):
            values = jnp.where((fine >> bit) & 1 == 1, pltpu.roll(values, 1 << bit, 1), values)
        out_ref[0, :, pl.ds(pl.multiple_of(i * step, 128), step)] = values[:, 128:].astype(out_ref.dtype)
        return carry

    lax.fori_loop(0, total_len // step, chunk, 0)


def shift(volts, delays):
    parts, rows, total_len = volts.shape
    block = pl.BlockSpec((1, rows, total_len), lambda i: (i, 0, 0))
    return pl.pallas_call(
        shift_kernel,
        grid=(parts,),
        in_specs=[pl.BlockSpec(memory_space=pltpu.SMEM), block],
        out_specs=block,
        out_shape=jax.ShapeDtypeStruct(volts.shape, volts.dtype),
        scratch_shapes=[
            pltpu.VMEM((rows, 2 * total_len), jnp.float32),
            pltpu.VMEM((rows, 2048 + 128), jnp.float32),
        ],
    )(delays, volts)


def split(values):
    high = values.astype(jnp.bfloat16)
    return high, (values - high.astype(jnp.float32)).astype(jnp.bfloat16)


def dot3(a_high, a_low, b_high, b_low):
    dot = functools.partial(jnp.dot, preferred_element_type=jnp.float32)
    return dot(a_high, b_high) + (dot(a_high, b_low) + dot(a_low, b_high))


def dedisperse_kernel(x_ref, h_real_ref, h_imag_ref, left_ref, right_ref, twist_ref, out_ref, flat):
    root = twist_ref.shape[1]
    half = root // 2
    cos_twist, sin_twist = twist_ref[0], twist_ref[1]
    x = x_ref[...].reshape(2 * root, root)
    a = dot3(left_ref[0], left_ref[1], *split(x))
    a_real, a_imag = a[:root], a[root:]
    b = jnp.concatenate(
        [a_real * cos_twist + a_imag * sin_twist, a_imag * cos_twist - a_real * sin_twist], axis=1
    )
    s = dot3(*split(b), right_ref[0], right_ref[1])
    s_real, s_imag = s[:, :root], s[:, root:]
    h_real, h_imag = h_real_ref[0], h_imag_ref[0]
    c = jnp.concatenate([s_real * h_real - s_imag * h_imag, s_real * h_imag + s_imag * h_real], axis=1)
    d = dot3(*split(c), left_ref[0], left_ref[1])
    d_real, d_imag = d[:, :root], d[:, root:]
    e = jnp.concatenate(
        [d_real * cos_twist - d_imag * sin_twist, d_imag * cos_twist + d_real * sin_twist], axis=0
    )
    out = dot3(right_ref[0], right_ref[1], *split(e)) * (1.0 / (root * root))
    for part in range(2):
        for side in range(2):
            flat[pl.ds(side, root, 2), :] = out[part * root : (part + 1) * root, side * half : (side + 1) * half]
        out_ref[:, part, 0] = flat[...].reshape(out_ref.shape[0], out_ref.shape[3], half)


def dedisperse(beams, h_real, h_imag, n_dev):
    _, n_beams, root, _ = beams.shape
    left, right, twist = dft_tables(root)
    rows = 2 * root // n_dev
    whole = lambda shape: pl.BlockSpec(shape, lambda b: (0,) * len(shape))
    own = pl.BlockSpec((1, root, root), lambda b: (b, 0, 0))
    return pl.pallas_call(
        dedisperse_kernel,
        grid=(n_beams,),
        in_specs=[
            pl.BlockSpec((2, 1, root, root), lambda b: (0, b, 0, 0)),
            own,
            own,
            whole(left.shape),
            whole(right.shape),
            whole(twist.shape),
        ],
        out_specs=pl.BlockSpec((n_dev, 2, 1, rows, root // 2), lambda b: (0, 0, b, 0, 0)),
        out_shape=jax.ShapeDtypeStruct((n_dev, 2, n_beams, rows, root // 2), jnp.float32),
        scratch_shapes=[pltpu.VMEM((2 * root, root // 2), jnp.float32)],
        cost_estimate=pl.CostEstimate(
            flops=96 * n_beams * root**3, bytes_accessed=24 * n_beams * root**2, transcendentals=0
        ),
    )(beams, h_real, h_imag, left, right, twist)


def shards(voltages, beam_weights, station_delays, dm_index):
    sub_dev = voltages.shape[0]
    total_len = voltages.shape[3]
    local_beams = dm_index.shape[0]
    trials = dm_index.shape[1]
    root_len = int(round(total_len**0.5))
    n_sub = lax.axis_size("sub")
    n_sta = lax.axis_size("sta")
    n_dev = n_sub * n_sta
    assert sub_dev == 1 and trials == 1 and root_len * root_len == total_len
    gathered = [
        lax.all_gather(shift(voltages[0, part : part + 1], station_delays)[0], "sta", axis=0, tiled=True)
        for part in range(2)
    ]
    own_weights = lax.dynamic_slice_in_dim(
        beam_weights, lax.axis_index("sta") * local_beams, local_beams, 2
    )[0]
    w_real, w_imag = own_weights[0], own_weights[1]
    weights = jnp.stack(
        [jnp.concatenate([w_real, w_imag], axis=0), jnp.concatenate([-w_imag, w_real], axis=0)]
    )
    beams = form_beams(weights, *gathered, root_len).reshape(2, local_beams, root_len, root_len)
    subband = lax.axis_index("sub") + jnp.arange(1, dtype=jnp.int32)
    base_phase = chirp_base(subband, root_len, total_len)
    dm_value = DM_STEP * dm_index.astype(jnp.float32)
    phase_table = dm_value[:, :, None] * base_phase
    sent = dedisperse(beams, jnp.cos(phase_table), jnp.sin(phase_table), n_dev)
    power = jnp.mean(beams[0] * beams[0] + beams[1] * beams[1], axis=(1, 2))
    rms = jnp.where(power > 0, jnp.sqrt(power), 1.0)
    gain = 32768.0 / root_len / rms
    undo = lax.all_gather(rms * (root_len / 32768.0), ("sub", "sta"), axis=0)
    sent = (sent * gain[None, None, :, None, None]).astype(jnp.float16)
    moved = lax.all_to_all(sent, ("sub", "sta"), split_axis=0, concat_axis=0, tiled=True)
    moved = moved.astype(jnp.float32) * undo[:, None, :, None, None]
    moved = moved.reshape(n_sub, n_sta, *moved.shape[1:]).transpose(0, 2, 1, 3, 4, 5)
    moved = moved.reshape(n_sub, 2, n_sta * local_beams, *moved.shape[4:])
    intensity = jnp.mean(moved[:, 0] * moved[:, 0] + moved[:, 1] * moved[:, 1], axis=0)
    return (moved.reshape(*moved.shape[:3], 1, -1), intensity.reshape(intensity.shape[0], 1, -1))


def solution(mesh):
    return jax.shard_map(
        shards,
        mesh=mesh,
        in_specs=(
            P("sub", None, "sta", None),
            P("sub", None, None, None),
            P("sta"),
            P("sta", None),
        ),
        out_specs=(P(None, None, None, None, ("sub", "sta")), P(None, None, ("sub", "sta"))),
        check_vma=False,
    )
```
